64 devices in a mesh: dp: 4 (over x, y), sp: 16 (over z, core).
Axes of the slice: x: 2, y: 2, z: 8, core: 2. Of those that a mesh axis runs over, the one named last changes fastest.
The devices are a block of a 4x4x8 slice.
Arguments:
- hidden: bfloat16 [64, 512, 2048], P('dp', 'sp'), parts along dimension 0
- pos_ids: int32 [64, 512], P('dp', 'sp'), parts along dimension 0
- block_ids: int32 [64, 512], P('dp', 'sp'), parts along dimension 0
- ctx_len: int32 [64], P('dp'), parts along dimension 0
- ln_gamma: bfloat16 [2048], replicated
- ln_beta: bfloat16 [2048], replicated
- w_qkv: bfloat16 [2048, 32, 3, 64], replicated
- b_qkv: bfloat16 [32, 3, 64], replicated
- w_dense: bfloat16 [2048, 2048], replicated
- b_dense: bfloat16 [2048], replicated
Outputs:
- output 1: bfloat16 [64, 512, 2048], P('dp', 'sp'), parts along dimension 0
- output 2: bfloat16 [64, 512, 32, 64], P('dp', None, 'sp'), parts along dimension 0
- output 3: bfloat16 [64, 512, 32, 64], P('dp', None, 'sp'), parts along dimension 0
There are 4 independent parts. The reference program is written for one: setup_inputs(seed, part) draws one part's arguments, and reference() takes and returns one part's arrays. A program takes and returns all parts, laid end to end along the dimension named above; an argument that names none is the same for every part.
All inputs are finite; a program needn't handle non-finite values.
Results may differ from the reference program's by a relative error of at most 0.00608031.
Values are sent between devices in bfloat16 or wider.
A program may use at most 768 MiB of HBM per device.

```python
import math
import jax
import jax.numpy as jnp
from jax import lax

BATCH = 16
SEQ = 512
HEADS = 32
HEAD = 64
HIDDEN = HEADS * HEAD
ALPHA = math.sqrt(56.0)
ROPE_BASE = 10000.0
LN_EPS = 1e-5
SCORE_SCALE = 1.0 / math.sqrt(HEAD)
QUERY_BLOCK = min(SEQ, 128)
GAIN = 1.0 / ALPHA
QKV_SCALE = ALPHA / math.sqrt(HIDDEN)
DENSE_SCALE = 0.5 * math.sqrt(SEQ / HIDDEN)
BIAS_SCALE = 1.0 / math.sqrt(SEQ)


def draw_positions(ctx_key, mask_key):
    ctx_len = jax.random.randint(ctx_key, (BATCH,), SEQ // 4, 3 * SEQ // 4 + 1, dtype=jnp.int32)
    mask_pos = jax.random.randint(mask_key, (BATCH,), 0, ctx_len, dtype=jnp.int32)
    token_pos = jnp.arange(SEQ, dtype=jnp.int32)[None, :]
    in_context = token_pos < ctx_len[:, None]
    pos_ids = jnp.where(in_context, token_pos, mask_pos[:, None]).astype(jnp.int32)
    block_ids = jnp.where(in_context, 0, token_pos - ctx_len[:, None] + 1).astype(jnp.int32)
    return pos_ids, block_ids, ctx_len


def setup_inputs(seed: int = 0, part: int = 0) -> dict:
    base_key = jax.random.key(seed)
    shared_key, part_key = jax.random.split(base_key)
    part_key = jax.random.fold_in(part_key, part)
    key_x, key_ctx, key_mask = jax.random.split(part_key, 3)
    key_g, key_b, key_w, key_wb, key_d, key_db = jax.random.split(shared_key, 6)
    pos_ids, block_ids, ctx_len = draw_positions(key_ctx, key_mask)
    hidden = jax.random.normal(key_x, (BATCH, SEQ, HIDDEN), jnp.float32)
    ln_gamma = (1.0 + 0.2 * jax.random.normal(key_g, (HIDDEN,), jnp.float32)) * GAIN
    ln_beta = jax.random.normal(key_b, (HIDDEN,), jnp.float32) * (GAIN * BIAS_SCALE)
    w_qkv = jax.random.normal(key_w, (HIDDEN, HEADS, 3, HEAD), jnp.float32) * QKV_SCALE
    b_qkv = jax.random.normal(key_wb, (HEADS, 3, HEAD), jnp.float32) * BIAS_SCALE
    w_dense = jax.random.normal(key_d, (HIDDEN, HIDDEN), jnp.float32) * DENSE_SCALE
    b_dense = jax.random.normal(key_db, (HIDDEN,), jnp.float32) * 0.5
    return {'hidden': hidden.astype(jnp.bfloat16), 'pos_ids': pos_ids, 'block_ids': block_ids, 'ctx_len': ctx_len, 'ln_gamma': ln_gamma.astype(jnp.bfloat16), 'ln_beta': ln_beta.astype(jnp.bfloat16), 'w_qkv': w_qkv.astype(jnp.bfloat16), 'b_qkv': b_qkv.astype(jnp.bfloat16), 'w_dense': w_dense.astype(jnp.bfloat16), 'b_dense': b_dense.astype(jnp.bfloat16)}


def layer_norm(hidden, ln_gamma, ln_beta):
    wide_in = hidden.astype(jnp.float32)
    row_mean = jnp.mean(wide_in, axis=-1, keepdims=True)
    centered = wide_in - row_mean
    row_var = jnp.mean(jnp.square(centered), axis=-1, keepdims=True)
    return (centered * lax.rsqrt(row_var + LN_EPS) * ln_gamma.astype(jnp.float32) + ln_beta.astype(jnp.float32)).astype(jnp.bfloat16)


def rotate(heads_in, pos_ids, block_ids):
    half_dim = heads_in.shape[-1] // 2
    quarter_dim = half_dim // 2
    inv_freq = ROPE_BASE ** (-jnp.arange(0, half_dim, 2).astype(jnp.float32) / half_dim)
    angles = jnp.stack([pos_ids, block_ids], axis=-1).astype(jnp.float32)[..., None] * inv_freq
    cos_a = jnp.cos(angles)[:, :, None]
    sin_a = jnp.sin(angles)[:, :, None]
    split_dims = heads_in.astype(jnp.float32).reshape(heads_in.shape[:-1] + (2, 2, quarter_dim))
    low_part = split_dims[..., 0, :]
    high_part = split_dims[..., 1, :]
    new_low = low_part * cos_a - high_part * sin_a
    new_high = high_part * cos_a + low_part * sin_a
    return jnp.stack([new_low, new_high], axis=-2).reshape(heads_in.shape).astype(jnp.bfloat16)


def reference(hidden, pos_ids, block_ids, ctx_len, ln_gamma, ln_beta, w_qkv, b_qkv, w_dense, b_dense):
    normed = layer_norm(hidden, ln_gamma, ln_beta)
    qkv_flat = jnp.dot(normed.reshape(BATCH * SEQ, HIDDEN), w_qkv.reshape(HIDDEN, 3 * HIDDEN), preferred_element_type=jnp.float32)
    qkv_proj = (qkv_flat.reshape(BATCH, SEQ, HEADS, 3, HEAD) + b_qkv.astype(jnp.float32)).astype(jnp.bfloat16)
    query_rot = rotate(qkv_proj[:, :, :, 0], pos_ids, block_ids)
    key_rot = rotate(qkv_proj[:, :, :, 1], pos_ids, block_ids)
    value_heads = qkv_proj[:, :, :, 2]
    key_pos = jnp.arange(SEQ)
    ctx_visible = key_pos[None, None, :] < ctx_len[:, None, None]

    def one_head(head_args):
        q_head, k_head, v_head = head_args
        k_wide = k_head.astype(jnp.float32)
        v_wide = v_head.astype(jnp.float32)

        def one_block(block_idx):
            block_start = block_idx * QUERY_BLOCK
            q_block = lax.dynamic_slice_in_dim(q_head, block_start, QUERY_BLOCK, axis=1).astype(jnp.float32)
            scores = jnp.einsum('bqe,bke->bqk', q_block, k_wide) * SCORE_SCALE
            q_pos = block_start + jnp.arange(QUERY_BLOCK)
            visible = ctx_visible | (key_pos[None, None, :] <= q_pos[None, :, None])
            attn_probs = jax.nn.softmax(jnp.where(visible, scores, -jnp.inf), axis=-1).astype(jnp.bfloat16)
            return jnp.einsum('bqk,bke->bqe', attn_probs.astype(jnp.float32), v_wide).astype(jnp.bfloat16)

        blocks = lax.map(one_block, jnp.arange(SEQ // QUERY_BLOCK))
        return jnp.moveaxis(blocks, 0, 1).reshape(BATCH, SEQ, HEAD)

    head_major = (jnp.moveaxis(query_rot, 2, 0), jnp.moveaxis(key_rot, 2, 0), jnp.moveaxis(value_heads, 2, 0))
    context = lax.map(one_head, head_major)
    context = jnp.moveaxis(context, 0, 2).reshape(BATCH * SEQ, HIDDEN)
    dense_out = jnp.dot(context, w_dense, preferred_element_type=jnp.float32) + b_dense.astype(jnp.float32)
    block_out = (normed.reshape(BATCH * SEQ, HIDDEN).astype(jnp.float32) * ALPHA + dense_out).astype(jnp.bfloat16)
    return block_out.reshape(BATCH, SEQ, HIDDEN), key_rot, value_heads
```

```python
import functools
import math

import jax
import jax.numpy as jnp
from jax import lax
from jax.experimental import pallas as pl
from jax.experimental.pallas import tpu as pltpu
from jax.sharding import PartitionSpec as P

ALPHA = math.sqrt(56.0)
ROPE_BASE = 10000.0
LN_EPS = 1e-5
CORES = 2
CHUNKS = 4
LANES = 128
QUERY_TILE = 128
CTX_MIN = 128
CTX_MAX = 384
LN_ROWS = 32
DENSE_COLS = 512
MESH = pl.DeviceIdType.MESH
NT = (((1,), (1,)), ((), ()))


def ring_order(n):
    order = []
    for step in range(1, n // 2):
        order += [step, n - step]
    return order + [n // 2]


def block_kernel(n, rows, toks, dh, hidden, w_hbm, b_qkv, wd_hbm, vecs, ctx, last_pos, freq,
                 out, k_out, v_out,
                 w_v, wd_v, a_v, fwd, qkv, cs, cr, ob, kvs, m_v,
                 h_sem, w_sem, wd_sem, a_send, a_recv, f_send, q_recv, c_send, c_recv, m_send, m_recv, kv_sem, o_sem):
    me = lax.axis_index('sp')
    chips = n // CORES
    chip, core = me // CORES, me % CORES
    part = rows // CHUNKS
    chunk = part * toks
    width = a_v.shape[2]
    seq = n * toks
    hl = w_hbm.shape[1]

    def device(chip_index, core_index):
        return {'sp': (chip_index % chips) * CORES + core_index}

    hidden_copies = []
    for k in range(CHUNKS):
        copy = pltpu.make_async_copy(hidden.at[pl.ds(k * chunk, chunk)], a_v.at[0, pl.ds(k * chunk, chunk)], h_sem.at[k])
        copy.start()
        hidden_copies.append(copy)

    def weight_copy(slot, block):
        for h in range(hl):
            for t in range(3):
                pltpu.make_async_copy(w_hbm.at[block, h, t], w_v.at[slot, t, h], w_sem.at[slot]).start()

    weight_blocks = [(0, 0), (0, 1), (1, 0), (1, 1), (2, 0), (2, 1), (-1, 0), (-1, 1), (-2, 0), (-2, 1), (3, 0), (-3, 1)]
    for slot, (step, kore) in enumerate(weight_blocks):
        weight_copy(slot, ((chip + step + chips) % chips) * CORES + kore)
    wd_copy = pltpu.make_async_copy(wd_hbm, wd_v, wd_sem)
    wd_copy.start()

    barrier = pltpu.get_barrier_semaphore()
    for step in range(1, n):
        pl.semaphore_signal(barrier, inc=1, device_id={'sp': (me + step) % n}, device_id_type=MESH)
    pl.semaphore_wait(barrier, n - 1)

    @pl.when(me == n - 1)
    def _():
        for step in range(1, n):
            pltpu.make_async_remote_copy(src_ref=last_pos, dst_ref=m_v, send_sem=m_send.at[step], recv_sem=m_recv,
                                         device_id={'sp': (me + step) % n}, device_id_type=MESH).start()

    def a_copy(k, side):
        peer = device(chip + 1 - 2 * side + chips, core)
        return pltpu.make_async_remote_copy(src_ref=a_v.at[0, pl.ds(k * chunk, chunk)],
                                            dst_ref=a_v.at[1 + side, pl.ds(k * chunk, chunk)],
                                            send_sem=a_send.at[side, k], recv_sem=a_recv.at[side, k],
                                            device_id=peer, device_id_type=MESH)

    gamma = vecs[0:1, :]
    beta = vecs[1:2, :]
    for k in range(CHUNKS):
        hidden_copies[k].wait()

        def norm_rows(i, carry):
            at = pl.ds(pl.multiple_of(k * chunk + i * LN_ROWS, LN_ROWS), LN_ROWS)
            x = a_v[0, at, :].astype(jnp.float32)
            mean = jnp.mean(x, axis=-1, keepdims=True)
            centered = x - mean
            var = jnp.mean(jnp.square(centered), axis=-1, keepdims=True)
            a_v[0, at, :] = (centered * lax.rsqrt(var + LN_EPS) * gamma + beta).astype(jnp.bfloat16)
            return carry

        lax.fori_loop(0, chunk // LN_ROWS, norm_rows, 0)
        for side in range(2):
            a_copy(k, side).start()

    def project(source, k, slot, count, block):
        a = a_v[source, pl.ds(pl.multiple_of(k * chunk, chunk), chunk), :]
        w = w_v[pl.ds(slot, count)].reshape(count * 3 * hl * dh, width)
        acc = lax.dot_general(a, w, NT, preferred_element_type=jnp.float32)
        cols = 3 * hl * dh
        return [(acc[:, i * cols:(i + 1) * cols] + b_qkv[block + i]).astype(jnp.bfloat16).reshape(part, toks, cols) for i in range(count)]

    def owner_at(k, owner):
        return pl.ds(k * part, part), pl.ds(pl.multiple_of(owner * toks, toks), toks)

    def send(value, k, slot, owner, dest):
        fwd[slot, k] = value
        at = owner_at(k, owner)
        pltpu.make_async_remote_copy(src_ref=fwd.at[slot, k], dst_ref=qkv.at[at[0], at[1]], send_sem=f_send, recv_sem=q_recv.at[k],
                                     device_id=dest, device_id_type=MESH).start()

    def to_own_chip(source, k, owner):
        values = project(source, k, 0, CORES, chip * CORES)
        for h in range(CORES):
            @pl.when(core == h)
            def _():
                at = owner_at(k, owner)
                qkv[at[0], at[1], :] = values[h]
                send(values[CORES - 1 - h], k, source, owner, device(chip, CORES - 1 - h))

    def wait_weights(slot):
        pltpu.make_async_copy(w_v.at[slot], w_v.at[slot], w_sem.at[slot]).wait()

    for slot in range(CORES):
        wait_weights(slot)

    def own_chunk(k, carry):
        to_own_chip(0, k, me)
        return carry

    lax.fori_loop(0, CHUNKS, own_chunk, 0)
    for slot in range(CORES, len(weight_blocks)):
        wait_weights(slot)

    def neighbour(side):
        return ((chip - 1 + 2 * side + chips) % chips) * CORES + core

    def forward_chunk(k, carry):
        for side in range(2):
            a_copy(k, side).wait_recv()

        def pair(index, c):
            side, step = index // 2, index % 2 + 1
            owner = neighbour(side)
            target = (chip + (1 - 2 * side) * step + chips) % chips
            values = project(1 + side, k, CORES + CORES * index, CORES, target * CORES)
            for h in range(CORES):
                send(values[h], k, 3 + CORES * index + h, owner, device(target, h))
            return c

        def single(side, c):
            owner = neighbour(side)
            target = (chip + (1 - 2 * side) * 3 + chips) % chips
            values = project(1 + side, k, 10 + side, 1, target * CORES + side)
            send(values[0], k, 11 + side, owner, device(target, side))
            return c

        def own(side, c):
            to_own_chip(1 + side, k, neighbour(side))
            return c

        lax.fori_loop(0, 4, pair, 0)
        lax.fori_loop(0, 2, single, 0)
        lax.fori_loop(0, 2, own, 0)
        return carry

    lax.fori_loop(0, CHUNKS, forward_chunk, 0)

    @pl.when(me == n - 1)
    def _():
        m_v[...] = last_pos[...]

    @pl.when(me != n - 1)
    def _():
        pltpu.make_async_copy(last_pos, m_v, m_recv).wait()

    row_iota = lax.broadcasted_iota(jnp.int32, (seq, LANES), 0)
    lane = lax.broadcasted_iota(jnp.int32, (seq, LANES), 1)
    pair_low = lane % (dh // 2) < dh // 4
    by_pos = lane % dh < dh // 2
    n_tiles = seq // QUERY_TILE

    def attend_row(b):
        ctx_b = ctx[pl.ds(b, 1), :]
        in_ctx = row_iota < ctx_b
        pos = jnp.where(in_ctx, row_iota.astype(jnp.float32), m_v[pl.ds(b, 1), :])
        blk = jnp.where(in_ctx, 0, row_iota - ctx_b + 1).astype(jnp.float32)
        angle = jnp.where(by_pos, pos, blk) * freq[...]
        cos = jnp.cos(angle)
        sin = jnp.sin(angle)
        sin = jnp.where(pair_low, -sin, sin)

        def rotate(x):
            swapped = jnp.where(pair_low, pltpu.roll(x, LANES - dh // 4, 1), pltpu.roll(x, dh // 4, 1))
            return x * cos + swapped * sin

        q = rotate(qkv[b, :, 0:LANES].astype(jnp.float32)) * (1.0 / math.sqrt(dh))
        k = rotate(qkv[b, :, LANES:2 * LANES].astype(jnp.float32))
        v_raw = qkv[b, :, 2 * LANES:3 * LANES]
        v = v_raw.astype(jnp.float32)
        slot = b % 2

        @pl.when(b >= 2)
        def _():
            pltpu.make_async_copy(kvs.at[slot], kvs.at[slot], kv_sem.at[slot]).wait()

        kvs[slot, 0] = k.astype(jnp.bfloat16).T
        kvs[slot, 1] = v_raw.T
        pltpu.make_async_copy(kvs.at[slot, 0], k_out.at[b], kv_sem.at[slot]).start()
        pltpu.make_async_copy(kvs.at[slot, 1], v_out.at[b], kv_sem.at[slot]).start()

        heads = []
        for h in range(hl):
            mine = lane // dh == h
            heads.append([jnp.where(mine, x, 0.0).astype(jnp.bfloat16) for x in (q, k, v)])
        for qt in range(n_tiles):
            start = qt * QUERY_TILE
            rows_here = slice(start, start + QUERY_TILE)
            keys_here = max(CTX_MAX, start + QUERY_TILE)
            bound = jnp.maximum(ctx_b, row_iota[rows_here] + 1)
            total = None
            for q_h, k_h, v_h in heads:
                s = lax.dot_general(q_h[rows_here], k_h[:keys_here], NT, preferred_element_type=jnp.float32)
                tiles = []
                for kt in range(keys_here // LANES):
                    tile = s[:, kt * LANES:(kt + 1) * LANES]
                    last_key = (kt + 1) * LANES - 1
                    if last_key >= CTX_MIN and last_key > start:
                        tile = jnp.where(lane[rows_here] + kt * LANES < bound, tile, -jnp.inf)
                    tiles.append(tile)
                top = functools.reduce(jnp.maximum, tiles)
                top = jnp.max(top, axis=-1, keepdims=True)
                tiles = [jnp.exp(tile - top) for tile in tiles]
                norm = jnp.sum(functools.reduce(jnp.add, tiles), axis=-1, keepdims=True)
                inv = 1.0 / norm
                probs = jnp.concatenate([(tile * inv).astype(jnp.bfloat16) for tile in tiles], axis=1)
                o = jnp.dot(probs, v_h[:keys_here], preferred_element_type=jnp.float32)
                total = o if total is None else total + o
            owners = QUERY_TILE // toks
            cs[pl.ds(qt * owners, owners), b] = total.astype(jnp.bfloat16).reshape(owners, toks, LANES)

    def attend_chunk(kk, carry):
        some = qkv.at[pl.ds(kk * part, part), pl.ds(0, 13 * toks)]
        pltpu.make_async_copy(some, some, q_recv.at[kk]).wait()

        def one_row(r, c):
            attend_row(kk * part + r)
            return c

        lax.fori_loop(0, part, one_row, 0)
        rows_k = pl.ds(kk * part, part)
        cols_me = pl.ds(pl.multiple_of(me * LANES, LANES), LANES)
        for step in ring_order(n):
            dest = (me + step) % n
            pltpu.make_async_remote_copy(src_ref=cs.at[dest, rows_k], dst_ref=cr.at[rows_k, :, cols_me], send_sem=c_send,
                                         recv_sem=c_recv.at[kk], device_id={'sp': dest}, device_id_type=MESH).start()
        cr[rows_k, :, cols_me] = cs[me, rows_k]
        return carry

    lax.fori_loop(0, CHUNKS, attend_chunk, 0)
    wd_copy.wait()

    def out_copy(kk, slot):
        return pltpu.make_async_copy(ob.at[slot], out.at[pl.ds(pl.multiple_of(kk * chunk, chunk), chunk)], o_sem.at[slot])

    def dense_chunk(kk, carry):
        some = cr.at[pl.ds(kk * part, part), :, pl.ds(0, (n - 1) * LANES)]
        pltpu.make_async_copy(some, some, c_recv.at[kk]).wait()
        slot = kk % 2

        @pl.when(kk >= 2)
        def _():
            out_copy(kk - 2, slot).wait()

        def columns(j, c):
            at = pl.ds(pl.multiple_of(j * DENSE_COLS, DENSE_COLS), DENSE_COLS)
            x = cr[pl.ds(kk * part, part)].reshape(chunk, width)
            dense = jnp.dot(x, wd_v[:, at], preferred_element_type=jnp.float32) + vecs[2:3, at]
            a = a_v[0, pl.ds(pl.multiple_of(kk * chunk, chunk), chunk), at].astype(jnp.float32)
            ob[slot, :, at] = (a * ALPHA + dense).astype(jnp.bfloat16)
            return c

        lax.fori_loop(0, width // DENSE_COLS, columns, 0)
        out_copy(kk, slot).start()
        return carry

    lax.fori_loop(0, CHUNKS, dense_chunk, 0)

    for kk in range(CHUNKS - 2, CHUNKS):
        out_copy(kk, kk % 2).wait()
    for slot in range(2):
        pltpu.make_async_copy(kvs.at[slot], kvs.at[slot], kv_sem.at[slot]).wait()
    for k in range(CHUNKS):
        for side in range(2):
            a_copy(k, side).wait_send()
    pltpu.make_async_copy(fwd, fwd, f_send).wait()
    sent = cs.at[pl.ds(0, n - 1)]
    pltpu.make_async_copy(sent, sent, c_send).wait()

    @pl.when(me == n - 1)
    def _():
        for step in range(1, n):
            pltpu.make_async_copy(last_pos, m_v, m_send.at[step]).wait()


def solution(mesh):
    n = mesh.shape['sp']
    seq_spec = P('dp', 'sp', None)
    row_spec = P('dp', 'sp')
    head_spec = P('dp', None, 'sp', None)
    replicated = P()

    def local_block(hidden, pos_ids, block_ids, ctx_len, ln_gamma, ln_beta, w_qkv, b_qkv, w_dense, b_dense):
        rows, toks, width = hidden.shape
        heads, _, dh = b_qkv.shape
        hl = heads // n
        seq = n * toks
        tokens = rows * toks
        part = rows // CHUNKS
        cols = 3 * hl * dh
        w_t = jnp.transpose(w_qkv, (1, 2, 3, 0)).reshape(n, hl, 3, dh, width)
        bias = jnp.transpose(b_qkv.astype(jnp.float32).reshape(n, hl, 3, dh), (0, 2, 1, 3)).reshape(n, 1, cols)
        vecs = jnp.stack([ln_gamma, ln_beta, b_dense]).astype(jnp.float32)
        ctx = jnp.broadcast_to(ctx_len[:, None], (rows, LANES))
        last_pos = jnp.broadcast_to(pos_ids[:, -1:].astype(jnp.float32), (rows, LANES))
        half = dh // 2
        inv_freq = ROPE_BASE ** (-jnp.arange(0, half, 2).astype(jnp.float32) / half)
        freq = jnp.tile(inv_freq, LANES // inv_freq.shape[0])[None, :]
        vmem = pl.BlockSpec(memory_space=pltpu.VMEM)
        anywhere = pl.BlockSpec(memory_space=pl.ANY)
        out, k_out, v_out = pl.pallas_call(
            functools.partial(block_kernel, n, rows, toks, dh),
            out_shape=[jax.ShapeDtypeStruct((tokens, width), jnp.bfloat16)] + [jax.ShapeDtypeStruct((rows, hl * dh, seq), jnp.bfloat16)] * 2,
            in_specs=[anywhere, anywhere, vmem, anywhere, vmem, vmem, vmem, vmem],
            out_specs=[anywhere] * 3,
            scratch_shapes=[
                pltpu.VMEM((12, 3, hl, dh, width), jnp.bfloat16),
                pltpu.VMEM((width, width), jnp.bfloat16),
                pltpu.VMEM((3, tokens, width), jnp.bfloat16),
                pltpu.VMEM((13, CHUNKS, part, toks, cols), jnp.bfloat16),
                pltpu.VMEM((rows, seq, cols), jnp.bfloat16),
                pltpu.VMEM((n, rows, toks, LANES), jnp.bfloat16),
                pltpu.VMEM((rows, toks, width), jnp.bfloat16),
                pltpu.VMEM((2, part * toks, width), jnp.bfloat16),
                pltpu.VMEM((2, 2, hl * dh, seq), jnp.bfloat16),
                pltpu.VMEM((rows, LANES), jnp.float32),
                pltpu.SemaphoreType.DMA((CHUNKS,)),
                pltpu.SemaphoreType.DMA((12,)),
                pltpu.SemaphoreType.DMA,
                pltpu.SemaphoreType.DMA((2, CHUNKS)),
                pltpu.SemaphoreType.DMA((2, CHUNKS)),
                pltpu.SemaphoreType.DMA,
                pltpu.SemaphoreType.DMA((CHUNKS,)),
                pltpu.SemaphoreType.DMA,
                pltpu.SemaphoreType.DMA((CHUNKS,)),
                pltpu.SemaphoreType.DMA((n,)),
                pltpu.SemaphoreType.DMA,
                pltpu.SemaphoreType.DMA((2,)),
                pltpu.SemaphoreType.DMA((2,)),
            ],
            compiler_params=pltpu.CompilerParams(collective_id=0, has_side_effects=True, vmem_limit_bytes=66_000_000),
            name='attention_block',
        )(hidden.reshape(tokens, width), w_t, bias, w_dense, vecs, ctx, last_pos, freq)

        def to_heads(x):
            return jnp.transpose(x.reshape(rows, hl, dh, seq), (0, 3, 1, 2))

        return out.reshape(rows, toks, width), to_heads(k_out), to_heads(v_out)

    return jax.shard_map(local_block, mesh=mesh, in_specs=(seq_spec, row_spec, row_spec, P('dp'), replicated, replicated, replicated, replicated, replicated, replicated), out_specs=(seq_spec, head_spec, head_spec), check_vma=False)
```

```python
import functools
import math

import jax
import jax.numpy as jnp
import numpy as np
from jax import lax
from jax.experimental import pallas as pl
from jax.experimental.pallas import tpu as pltpu
from jax.sharding import PartitionSpec as P

ALPHA = math.sqrt(56.0)
ROPE_BASE = 10000.0
LN_EPS = 1e-5
CORES = 2
CHUNKS = 4
LANES = 128
QUERY_TILE = 128
CTX_MIN = 128
CTX_MAX = 384
FIRST_ROWS = 4
DENSE_COLS = 512
MESH = pl.DeviceIdType.MESH
NT = (((1,), (1,)), ((), ()))


def far_first(n):
    half = n // 2
    order = [half]
    for step in range(1, half):
        order += [half - step, half + step]
    return order


def block_kernel(n, rows, toks, dh, hidden, w_hbm, bq_hbm, wd_hbm, gamma_hbm, beta_hbm, bd_hbm, ctx_hbm, pos_hbm, freq_hbm,
                 out_v, k_v, v_v, wd_v, last_v, rest_v,
                 w_v, a_v, fwd, qkv, cs, cr, bq_v, bias, g_v, be_v, bd_v, vecs, ctx, pos_v, m_v, freq,
                 h_sem, w_sem, wd_sem, small_sem, a_send, a_recv, f_send, q_recv, c_send, c_recv, m_send, m_recv):
    me = lax.axis_index('sp')
    chips = n // CORES
    chip, core = me // CORES, me % CORES
    part = rows // CHUNKS
    chunk = part * toks
    width = a_v.shape[2]
    seq = n * toks
    hl = w_hbm.shape[1]

    def device(chip_index, core_index):
        return {'sp': (chip_index % chips) * CORES + core_index}

    barrier = pltpu.get_barrier_semaphore()
    for step in range(1, n):
        pl.semaphore_signal(barrier, inc=1, device_id={'sp': (me + step) % n}, device_id_type=MESH)

    def row_at(r):
        return pl.ds(pl.multiple_of(r * toks, toks), toks)

    def hidden_copy(r):
        return pltpu.make_async_copy(hidden.at[row_at(r)], a_v.at[0, row_at(r)], h_sem.at[r])

    small = [(gamma_hbm, g_v), (beta_hbm, be_v), (bd_hbm, bd_v), (bq_hbm, bq_v), (ctx_hbm, ctx), (pos_hbm, pos_v), (freq_hbm, freq)]
    small_copies = [pltpu.make_async_copy(src, dst, small_sem.at[i]) for i, (src, dst) in enumerate(small)]
    for copy in small_copies[:2]:
        copy.start()
    for r in range(rows):
        hidden_copy(r).start()
    for copy in small_copies[2:]:
        copy.start()
    for i in range(2):
        small_copies[i].wait()
        vecs[i:i + 1, :] = small[i][1][...].astype(jnp.float32)[None, :]
    pl.semaphore_wait(barrier, n - 1)

    def a_copy(start, size, k, side):
        peer = device(chip + 1 - 2 * side + chips, core)
        at = pl.ds(start, size)
        return pltpu.make_async_remote_copy(src_ref=a_v.at[0, at], dst_ref=a_v.at[1 + side, at],
                                            send_sem=a_send.at[side], recv_sem=a_recv.at[side, k],
                                            device_id=peer, device_id_type=MESH)

    def norm_row(r, carry):
        hidden_copy(r).wait()
        x = a_v[0, row_at(r), :].astype(jnp.float32)
        mean = jnp.mean(x, axis=-1, keepdims=True)
        centered = x - mean
        var = jnp.mean(jnp.square(centered), axis=-1, keepdims=True)
        a_v[0, row_at(r), :] = (centered * lax.rsqrt(var + LN_EPS) * vecs[0:1, :] + vecs[1:2, :]).astype(jnp.bfloat16)
        for side in range(2):
            a_copy(pl.multiple_of(r * toks, toks), toks, r // part, side).start()
        return carry

    lax.fori_loop(0, FIRST_ROWS, norm_row, 0)

    def weight_copy(slot, block):
        for h in range(hl):
            for t in range(3):
                pltpu.make_async_copy(w_hbm.at[block, h, t], w_v.at[slot, t, h], w_sem.at[slot]).start()

    weight_blocks = [(0, 0), (0, 1), (1, 0), (1, 1), (2, 0), (2, 1), (-1, 0), (-1, 1), (-2, 0), (-2, 1), (3, 0), (-3, 1)]
    for slot, (step, kore) in enumerate(weight_blocks):
        weight_copy(slot, ((chip + step + chips) % chips) * CORES + kore)
    wd_copy = pltpu.make_async_copy(wd_hbm, wd_v, wd_sem)
    wd_copy.start()
    lax.fori_loop(FIRST_ROWS, rows, norm_row, 0)

    for copy in small_copies[2:]:
        copy.wait()
    vecs[2:3, :] = bd_v[...].astype(jnp.float32)[None, :]
    raw = bq_v[...].astype(jnp.float32)
    for d in range(n):
        for t in range(3):
            bias[d, :, t * hl * dh:(t + 1) * hl * dh] = jnp.concatenate([raw[t, hl * d + h:hl * d + h + 1] for h in range(hl)], axis=1)

    @pl.when(me == n - 1)
    def _():
        for step in range(1, n):
            pltpu.make_async_remote_copy(src_ref=pos_v, dst_ref=m_v, send_sem=m_send.at[step], recv_sem=m_recv,
                                         device_id={'sp': (me + step) % n}, device_id_type=MESH).start()
        m_v[...] = pos_v[...]

    def project(source, k, slot, count, block):
        a = a_v[source, pl.ds(pl.multiple_of(k * chunk, chunk), chunk), :]
        w = w_v[pl.ds(slot, count)].reshape(count * 3 * hl * dh, width)
        acc = lax.dot_general(a, w, NT, preferred_element_type=jnp.float32)
        cols = 3 * hl * dh
        return [(acc[:, i * cols:(i + 1) * cols] + bias[block + i]).astype(jnp.bfloat16).reshape(part, toks, cols) for i in range(count)]

    def owner_at(k, owner):
        return pl.ds(k * part, part), pl.ds(pl.multiple_of(owner * toks, toks), toks)

    def send(value, k, slot, owner, dest):
        fwd[slot, k] = value
        at = owner_at(k, owner)
        pltpu.make_async_remote_copy(src_ref=fwd.at[slot, k], dst_ref=qkv.at[at[0], at[1]], send_sem=f_send, recv_sem=q_recv.at[k],
                                     device_id=dest, device_id_type=MESH).start()

    def to_own_chip(source, k, owner):
        values = project(source, k, 0, CORES, chip * CORES)
        for h in range(CORES):
            @pl.when(core == h)
            def _():
                at = owner_at(k, owner)
                qkv[at[0], at[1], :] = values[h]
                send(values[CORES - 1 - h], k, source, owner, device(chip, CORES - 1 - h))

    def wait_weights(slot):
        pltpu.make_async_copy(w_v.at[slot], w_v.at[slot], w_sem.at[slot]).wait()

    for slot in range(CORES):
        wait_weights(slot)

    def own_chunk(k, carry):
        to_own_chip(0, k, me)
        return carry

    lax.fori_loop(0, CHUNKS, own_chunk, 0)
    for slot in range(CORES, len(weight_blocks)):
        wait_weights(slot)

    def neighbour(side):
        return ((chip - 1 + 2 * side + chips) % chips) * CORES + core

    def forward_chunk(k, carry):
        for side in range(2):
            a_copy(pl.multiple_of(k * chunk, chunk), chunk, k, side).wait_recv()

        def single(side, c):
            owner = neighbour(side)
            target = (chip + (1 - 2 * side) * 3 + chips) % chips
            values = project(1 + side, k, 10 + side, 1, target * CORES + side)
            send(values[0], k, 11 + side, owner, device(target, side))
            return c

        def pair(i, c):
            side, step = i % 2, 2 - i // 2
            index = 2 * side + step - 1
            owner = neighbour(side)
            target = (chip + (1 - 2 * side) * step + chips) % chips
            values = project(1 + side, k, CORES + CORES * index, CORES, target * CORES)
            for h in range(CORES):
                send(values[h], k, 3 + CORES * index + h, owner, device(target, h))
            return c

        def own(side, c):
            to_own_chip(1 + side, k, neighbour(side))
            return c

        lax.fori_loop(0, 2, single, 0)
        lax.fori_loop(0, 4, pair, 0)
        lax.fori_loop(0, 2, own, 0)
        return carry

    lax.fori_loop(0, CHUNKS, forward_chunk, 0)

    @pl.when(me != n - 1)
    def _():
        pltpu.make_async_copy(pos_v, m_v, m_recv).wait()

    row_iota = lax.broadcasted_iota(jnp.int32, (seq, LANES), 0)
    lane = lax.broadcasted_iota(jnp.int32, (seq, LANES), 1)
    pair_low = lane % (dh // 2) < dh // 4
    by_pos = lane % dh < dh // 2
    n_tiles = seq // QUERY_TILE
    last_lane = lax.broadcasted_iota(jnp.int32, (1, toks), 1) == toks - 1

    def attend_row(b):
        ctx_b = ctx[b]
        m_b = jnp.sum(jnp.where(last_lane, m_v[pl.ds(b, 1), :].astype(jnp.float32), 0.0), axis=-1, keepdims=True)
        in_ctx = row_iota < ctx_b
        pos = jnp.where(in_ctx, row_iota.astype(jnp.float32), m_b)
        blk = jnp.where(in_ctx, 0, row_iota - ctx_b + 1).astype(jnp.float32)
        angle = jnp.where(by_pos, pos, blk) * freq[...]
        cos = jnp.cos(angle)
        sin = jnp.sin(angle)
        sin = jnp.where(pair_low, -sin, sin)

        def rotate(x):
            swapped = jnp.where(pair_low, pltpu.roll(x, LANES - dh // 4, 1), pltpu.roll(x, dh // 4, 1))
            return x * cos + swapped * sin

        q = rotate(qkv[b, :, 0:LANES].astype(jnp.float32)) * (1.0 / math.sqrt(dh))
        k = rotate(qkv[b, :, LANES:2 * LANES].astype(jnp.float32))
        v_raw = qkv[b, :, 2 * LANES:3 * LANES]
        v = v_raw.astype(jnp.float32)
        k_v[b] = k.astype(jnp.bfloat16).T
        v_v[b] = v_raw.T

        heads = []
        for h in range(hl):
            mine = lane // dh == h
            heads.append([jnp.where(mine, x, 0.0).astype(jnp.bfloat16) for x in (q, k, v)])
        for qt in range(n_tiles):
            start = qt * QUERY_TILE
            rows_here = slice(start, start + QUERY_TILE)
            keys_here = max(CTX_MAX, start + QUERY_TILE)
            bound = jnp.maximum(ctx_b, row_iota[rows_here] + 1)
            total = None
            for q_h, k_h, v_h in heads:
                s = lax.dot_general(q_h[rows_here], k_h[:keys_here], NT, preferred_element_type=jnp.float32)
                tiles = []
                for kt in range(keys_here // LANES):
                    tile = s[:, kt * LANES:(kt + 1) * LANES]
                    last_key = (kt + 1) * LANES - 1
                    if last_key >= CTX_MIN and last_key > start:
                        tile = jnp.where(lane[rows_here] + kt * LANES < bound, tile, -jnp.inf)
                    tiles.append(tile)
                top = functools.reduce(jnp.maximum, tiles)
                top = jnp.max(top, axis=-1, keepdims=True)
                tiles = [jnp.exp(tile - top) for tile in tiles]
                norm = jnp.sum(functools.reduce(jnp.add, tiles), axis=-1, keepdims=True)
                inv = 1.0 / norm
                probs = jnp.concatenate([(tile * inv).astype(jnp.bfloat16) for tile in tiles], axis=1)
                o = jnp.dot(probs, v_h[:keys_here], preferred_element_type=jnp.float32)
                total = o if total is None else total + o
            owners = QUERY_TILE // toks
            cs[pl.ds(qt * owners, owners), b] = total.astype(jnp.bfloat16).reshape(owners, toks, LANES)

    def attend_chunk(kk, carry):
        some = qkv.at[pl.ds(kk * part, part), pl.ds(0, 13 * toks)]
        pltpu.make_async_copy(some, some, q_recv.at[kk]).wait()

        def one_row(r, c):
            attend_row(kk * part + r)
            return c

        lax.fori_loop(0, part, one_row, 0)
        rows_k = pl.ds(kk * part, part)
        cols_me = pl.ds(pl.multiple_of(me * LANES, LANES), LANES)
        for step in far_first(n):
            dest = (me + step) % n
            pltpu.make_async_remote_copy(src_ref=cs.at[dest, rows_k], dst_ref=cr.at[rows_k, :, cols_me], send_sem=c_send,
                                         recv_sem=c_recv.at[kk], device_id={'sp': dest}, device_id_type=MESH).start()
        cr[rows_k, :, cols_me] = cs[me, rows_k]
        return carry

    lax.fori_loop(0, CHUNKS, attend_chunk, 0)
    wd_copy.wait()

    def context_wait(kk):
        some = cr.at[pl.ds(kk * part, part), :, pl.ds(0, (n - 1) * LANES)]
        pltpu.make_async_copy(some, some, c_recv.at[kk]).wait()

    def dense_chunk(kk, carry):
        context_wait(kk)

        def columns(j, c):
            at = pl.ds(pl.multiple_of(j * DENSE_COLS, DENSE_COLS), DENSE_COLS)
            here = pl.ds(pl.multiple_of(kk * chunk, chunk), chunk)
            x = cr[pl.ds(kk * part, part)].reshape(chunk, width)
            dense = jnp.dot(x, wd_v[:, at], preferred_element_type=jnp.float32) + vecs[2:3, at]
            out_v[here, at] = (a_v[0, here, at].astype(jnp.float32) * ALPHA + dense).astype(jnp.bfloat16)
            return c

        lax.fori_loop(0, width // DENSE_COLS, columns, 0)
        return carry

    lax.fori_loop(0, CHUNKS - 1, dense_chunk, 0)
    rest_v[...] = a_v[0, pl.ds((CHUNKS - 1) * chunk, chunk), :].astype(jnp.float32) * ALPHA + vecs[2:3, :]
    for side in range(2):
        whole = a_v.at[0]
        pltpu.make_async_copy(whole, whole, a_send.at[side]).wait()
    pltpu.make_async_copy(fwd, fwd, f_send).wait()

    @pl.when(me == n - 1)
    def _():
        for step in range(1, n):
            pltpu.make_async_copy(pos_v, m_v, m_send.at[step]).wait()

    sent = cs.at[pl.ds(0, n - 1)]
    pltpu.make_async_copy(sent, sent, c_send).wait()
    context_wait(CHUNKS - 1)
    last_v[...] = cr[pl.ds((CHUNKS - 1) * part, part)].reshape(chunk, width)


def finish_kernel(out_v, k_v, v_v, wd_v, last_v, rest_v, out, k_out, v_out, tail_v, sem, tail_sem):
    done = out_v.shape[0]
    chunk, width = last_v.shape
    copies = [pltpu.make_async_copy(k_v, k_out, sem.at[0]), pltpu.make_async_copy(v_v, v_out, sem.at[1]),
              pltpu.make_async_copy(out_v, out.at[pl.ds(0, done)], sem.at[2])]
    for copy in copies:
        copy.start()
    for j in range(width // DENSE_COLS):
        at = pl.ds(j * DENSE_COLS, DENSE_COLS)
        dense = jnp.dot(last_v[...], wd_v[:, at], preferred_element_type=jnp.float32)
        tail_v[:, at] = (rest_v[:, at] + dense).astype(jnp.bfloat16)
        copy = pltpu.make_async_copy(tail_v.at[:, at], out.at[pl.ds(done, chunk), at], tail_sem.at[j])
        copy.start()
        copies.append(copy)
    for copy in copies:
        copy.wait()


def solution(mesh):
    n = mesh.shape['sp']
    seq_spec = P('dp', 'sp', None)
    row_spec = P('dp', 'sp')
    head_spec = P('dp', None, 'sp', None)
    replicated = P()

    def local_block(hidden, pos_ids, block_ids, ctx_len, ln_gamma, ln_beta, w_qkv, b_qkv, w_dense, b_dense):
        rows, toks, width = hidden.shape
        heads, _, dh = b_qkv.shape
        hl = heads // n
        seq = n * toks
        tokens = rows * toks
        part = rows // CHUNKS
        chunk = part * toks
        cols = 3 * hl * dh
        bf16, f32 = jnp.bfloat16, jnp.float32
        w_t = jnp.transpose(w_qkv, (1, 2, 3, 0)).reshape(n, hl, 3, dh, width)
        half = dh // 2
        inv_freq = ROPE_BASE ** (-np.arange(0, half, 2).astype(np.float32) / half)
        freq = np.tile(inv_freq.astype(np.float32), LANES // inv_freq.shape[0])[None, :]
        vmem = pl.BlockSpec(memory_space=pltpu.VMEM)
        anywhere = pl.BlockSpec(memory_space=pl.ANY)
        kv_shape = (rows, hl * dh, seq)
        staged = pl.pallas_call(
            functools.partial(block_kernel, n, rows, toks, dh),
            out_shape=[pltpu.VMEM((tokens - chunk, width), bf16), pltpu.VMEM(kv_shape, bf16), pltpu.VMEM(kv_shape, bf16),
                       pltpu.VMEM((width, width), bf16), pltpu.VMEM((chunk, width), bf16), pltpu.VMEM((chunk, width), f32)],
            in_specs=[anywhere] * 10,
            out_specs=[vmem] * 6,
            scratch_shapes=[
                pltpu.VMEM((12, 3, hl, dh, width), bf16),
                pltpu.VMEM((3, tokens, width), bf16),
                pltpu.VMEM((13, CHUNKS, part, toks, cols), bf16),
                pltpu.VMEM((rows, seq, cols), bf16),
                pltpu.VMEM((n, rows, toks, LANES), bf16),
                pltpu.VMEM((rows, toks, width), bf16),
                pltpu.VMEM((3, heads, dh), bf16),
                pltpu.VMEM((n, 1, cols), f32),
                pltpu.VMEM((width,), bf16),
                pltpu.VMEM((width,), bf16),
                pltpu.VMEM((width,), bf16),
                pltpu.VMEM((8, width), f32),
                pltpu.SMEM((rows,), jnp.int32),
                pltpu.VMEM((rows, toks), jnp.int32),
                pltpu.VMEM((rows, toks), jnp.int32),
                pltpu.VMEM((1, LANES), f32),
                pltpu.SemaphoreType.DMA((rows,)),
                pltpu.SemaphoreType.DMA((12,)),
                pltpu.SemaphoreType.DMA,
                pltpu.SemaphoreType.DMA((7,)),
                pltpu.SemaphoreType.DMA((2,)),
                pltpu.SemaphoreType.DMA((2, CHUNKS)),
                pltpu.SemaphoreType.DMA,
                pltpu.SemaphoreType.DMA((CHUNKS,)),
                pltpu.SemaphoreType.DMA,
                pltpu.SemaphoreType.DMA((CHUNKS,)),
                pltpu.SemaphoreType.DMA((n,)),
                pltpu.SemaphoreType.DMA,
            ],
            compiler_params=pltpu.CompilerParams(collective_id=0, has_side_effects=True, vmem_limit_bytes=46 * 2**20),
            name='attention_block',
        )(hidden.reshape(tokens, width), w_t, jnp.transpose(b_qkv, (1, 0, 2)), w_dense, ln_gamma, ln_beta, b_dense, ctx_len, pos_ids, freq)
        out, k_out, v_out = pl.pallas_call(
            finish_kernel,
            out_shape=[jax.ShapeDtypeStruct((tokens, width), bf16)] + [jax.ShapeDtypeStruct(kv_shape, bf16)] * 2,
            in_specs=[vmem] * 6,
            out_specs=[anywhere] * 3,
            scratch_shapes=[pltpu.VMEM((chunk, width), bf16), pltpu.SemaphoreType.DMA((3,)), pltpu.SemaphoreType.DMA((width // DENSE_COLS,))],
            compiler_params=pltpu.CompilerParams(vmem_limit_bytes=4 * 2**20),
            name='finish_block',
        )(*staged)

        def to_heads(x):
            return jnp.transpose(x.reshape(rows, hl, dh, seq), (0, 3, 1, 2))

        return out.reshape(rows, toks, width), to_heads(k_out), to_heads(v_out)

    return jax.shard_map(local_block, mesh=mesh, in_specs=(seq_spec, row_spec, row_spec, P('dp'), replicated, replicated, replicated, replicated, replicated, replicated), out_specs=(seq_spec, head_spec, head_spec), check_vma=False)
```

```python
import functools
import math

import jax
import jax.numpy as jnp
import numpy as np
from jax import lax
from jax.experimental import pallas as pl
from jax.experimental.pallas import tpu as pltpu
from jax.sharding import PartitionSpec as P

ALPHA = math.sqrt(56.0)
ROPE_BASE = 10000.0
LN_EPS = 1e-5
CORES = 2
CHUNKS = 4
LANES = 128
QUERY_TILE = 128
CTX_MIN = 128
CTX_MAX = 384
FIRST_ROWS = 4
PLACES = 12
DENSE_COLS = 512
MESH = pl.DeviceIdType.MESH
NT = (((1,), (1,)), ((), ()))


def far_first(n):
    half = n // 2
    order = [half]
    for step in range(1, half):
        order += [half - step, half + step]
    return order


def block_kernel(n, rows, toks, dh, hidden, w_hbm, bq_hbm, wd_hbm, gamma_hbm, beta_hbm, bd_hbm, ctx_hbm, pos_hbm, freq_hbm,
                 out_v, k_v, v_v, wd_v, last_v, rest_v,
                 w_v, a_v, fwd, qkv, cs, cr, bq_v, bias, g_v, be_v, bd_v, vecs, ctx, pos_v, m_v, freq, table,
                 h_sem, w_sem, wd_sem, small_sem, a_send, a_recv, r_send, r_recv, f_send, q_recv, c_send, c_recv, m_send, m_recv):
    me = lax.axis_index('sp')
    chips = n // CORES
    chip, core = me // CORES, me % CORES
    part = rows // CHUNKS
    chunk = part * toks
    width = a_v.shape[2]
    seq = n * toks
    hl = w_hbm.shape[1]

    def device(chip_index, core_index):
        return {'sp': (chip_index % chips) * CORES + core_index}

    barrier = pltpu.get_barrier_semaphore()
    for step in range(1, n):
        pl.semaphore_signal(barrier, inc=1, device_id={'sp': (me + step) % n}, device_id_type=MESH)

    def row_at(r):
        return pl.ds(pl.multiple_of(r * toks, toks), toks)

    def hidden_copy(r):
        return pltpu.make_async_copy(hidden.at[row_at(r)], a_v.at[0, row_at(r)], h_sem.at[r])

    small = [(gamma_hbm, g_v), (beta_hbm, be_v), (bd_hbm, bd_v), (bq_hbm, bq_v), (ctx_hbm, ctx), (pos_hbm, pos_v), (freq_hbm, freq)]
    small_copies = [pltpu.make_async_copy(src, dst, small_sem.at[i]) for i, (src, dst) in enumerate(small)]
    for copy in small_copies[:2]:
        copy.start()
    for r in range(rows):
        hidden_copy(r).start()
    for copy in small_copies[2:]:
        copy.start()
    for i in range(2):
        small_copies[i].wait()
        vecs[i:i + 1, :] = small[i][1][...].astype(jnp.float32)[None, :]
    pl.semaphore_wait(barrier, n - 1)

    def a_copy(start, size, k, side):
        peer = device(chip + 1 - 2 * side + chips, core)
        at = pl.ds(start, size)
        return pltpu.make_async_remote_copy(src_ref=a_v.at[0, at], dst_ref=a_v.at[1 + side, at],
                                            send_sem=a_send.at[side], recv_sem=a_recv.at[side, k],
                                            device_id=peer, device_id_type=MESH)

    def norm_row(r, carry):
        hidden_copy(r).wait()
        x = a_v[0, row_at(r), :].astype(jnp.float32)
        mean = jnp.mean(x, axis=-1, keepdims=True)
        centered = x - mean
        var = jnp.mean(jnp.square(centered), axis=-1, keepdims=True)
        a_v[0, row_at(r), :] = (centered * lax.rsqrt(var + LN_EPS) * vecs[0:1, :] + vecs[1:2, :]).astype(jnp.bfloat16)
        return carry

    def norm_send_row(r, carry):
        norm_row(r, carry)
        for side in range(2):
            a_copy(pl.multiple_of(r * toks, toks), toks, r // part, side).start()
        return carry

    lax.fori_loop(0, FIRST_ROWS, norm_send_row, 0)

    def weight_copy(slot, block):
        for h in range(hl):
            for t in range(3):
                pltpu.make_async_copy(w_hbm.at[block, h, t], w_v.at[slot, t, h], w_sem.at[slot]).start()

    weight_blocks = [(step, kore) for step in (0, 1, 2, -1, -2) for kore in range(CORES)]
    for slot, (step, kore) in enumerate(weight_blocks):
        weight_copy(slot, ((chip + step + chips) % chips) * CORES + kore)
    wd_copy = pltpu.make_async_copy(wd_hbm, wd_v, wd_sem)
    wd_copy.start()
    lax.fori_loop(FIRST_ROWS, 2 * part, norm_send_row, 0)
    lax.fori_loop(2 * part, rows, norm_row, 0)

    for copy in small_copies[2:]:
        copy.wait()
    vecs[2:3, :] = bd_v[...].astype(jnp.float32)[None, :]
    raw = bq_v[...].astype(jnp.float32)
    for d in range(n):
        for t in range(3):
            bias[d, :, t * hl * dh:(t + 1) * hl * dh] = jnp.concatenate([raw[t, hl * d + h:hl * d + h + 1] for h in range(hl)], axis=1)

    @pl.when(me == n - 1)
    def _():
        for step in range(1, n):
            pltpu.make_async_remote_copy(src_ref=pos_v, dst_ref=m_v, send_sem=m_send.at[step], recv_sem=m_recv,
                                         device_id={'sp': (me + step) % n}, device_id_type=MESH).start()
        m_v[...] = pos_v[...]

    def project(source, k, slot, count, block):
        a = a_v[source, pl.ds(pl.multiple_of(k * chunk, chunk), chunk), :]
        w = w_v[pl.ds(slot, count)].reshape(count * 3 * hl * dh, width)
        acc = lax.dot_general(a, w, NT, preferred_element_type=jnp.float32)
        cols = 3 * hl * dh
        return [(acc[:, i * cols:(i + 1) * cols] + bias[block + i]).astype(jnp.bfloat16).reshape(part, toks, cols) for i in range(count)]

    def owner_at(k, owner):
        return pl.ds(k * part, part), pl.ds(pl.multiple_of(owner * toks, toks), toks)

    def send(value, k, slot, owner, dest):
        fwd[slot, k] = value
        at = owner_at(k, owner)
        pltpu.make_async_remote_copy(src_ref=fwd.at[slot, k], dst_ref=qkv.at[at[0], at[1]], send_sem=f_send, recv_sem=q_recv.at[k],
                                     device_id=dest, device_id_type=MESH).start()

    def job(source, k, slot, target, owner, place, apart, own):
        values = project(source, k, slot, CORES, target * CORES)
        for h in range(CORES):
            keep = jnp.logical_and(own == 1, core == h)

            @pl.when(keep)
            def _():
                at = owner_at(k, owner)
                qkv[at[0], at[1], :] = values[h]

            @pl.when(jnp.logical_not(keep))
            def _():
                send(values[h], k, place + h * apart, owner, device(target, h))

    def wait_weights(slot):
        pltpu.make_async_copy(w_v.at[slot], w_v.at[slot], w_sem.at[slot]).wait()

    table_rows = table.shape[1]

    def table_block(i, carry):
        at = pl.ds(pl.multiple_of(i * LANES, LANES), LANES)
        index = lax.broadcasted_iota(jnp.int32, (LANES, LANES), 0) + (i * LANES - seq)
        angle = jnp.maximum(index, 0).astype(jnp.float32) * freq[...]
        quarter = lax.broadcasted_iota(jnp.int32, (LANES, LANES), 1) % (dh // 2) < dh // 4
        sin = jnp.sin(angle)
        table[0, at, :] = jnp.cos(angle)
        table[1, at, :] = jnp.where(quarter, -sin, sin)
        return carry

    lax.fori_loop(0, table_rows // LANES, table_block, 0)
    for slot in range(CORES):
        wait_weights(slot)

    def chip_at(offset):
        return (chip + offset + chips) % chips

    def chunk_at(k):
        return pl.ds(pl.multiple_of(k * chunk, chunk), chunk)

    def own_chunk(k, carry):
        job(0, k, 0, chip, me, 0, 0, 1)
        return carry

    def relay(k):
        odd = k % 2
        return pltpu.make_async_remote_copy(src_ref=a_v.at[1 + odd, chunk_at(k)], dst_ref=a_v.at[3, chunk_at(k)],
                                            send_sem=r_send, recv_sem=r_recv.at[k],
                                            device_id=device(chip_at(1 - 2 * odd), core), device_id_type=MESH)

    def near_chunk(k, carry):
        odd = k % 2
        for side in range(2):
            a_copy(pl.multiple_of(k * chunk, chunk), chunk, k, side).wait_recv()
        relay(k).start()

        def one(i, c):
            own = i // 2
            step = (2 - i) * (1 - own)
            source = (1 - own) * (2 - odd) + own * ((3 - i) * (1 + odd) + (i - 2) * (2 - odd))
            slot = (1 - own) * (CORES + CORES * (2 * (1 - odd) + step - 1))
            place = (1 - own) * (4 + CORES * (step - 1)) + own * source
            owner = chip_at(2 * source - 3) * CORES + core
            job(source, k, slot, chip_at((2 * odd - 1) * step), owner, place, 1 - own, own)
            return c

        lax.fori_loop(0, 4, one, 0)
        return carry

    def far_chunk(k, carry):
        odd = k % 2
        there = a_v.at[3, chunk_at(k)]
        pltpu.make_async_copy(there, there, r_recv.at[k]).wait()
        owner = chip_at(4 * odd - 2) * CORES + core

        def one(i, c):
            own = i // 2
            step = 2 - i
            slot = (1 - own) * (CORES + CORES * (2 * odd + step - 1))
            place = (1 - own) * (8 + CORES * (step - 1)) + own * 3
            job(3, k, slot, chip_at((1 - 2 * odd) * step), owner, place, 1 - own, own)
            return c

        lax.fori_loop(0, 3, one, 0)
        return carry

    lax.fori_loop(0, CHUNKS, own_chunk, 0)
    for slot in range(CORES, len(weight_blocks)):
        wait_weights(slot)
    near_chunk(0, 0)
    for k in range(2, CHUNKS):
        for side in range(2):
            a_copy(k * chunk, chunk, k, side).start()
    near_chunk(1, 0)
    far_chunk(0, 0)
    lax.fori_loop(2, CHUNKS, near_chunk, 0)
    far_chunk(1, 0)

    @pl.when(me != n - 1)
    def _():
        pltpu.make_async_copy(pos_v, m_v, m_recv).wait()

    row_iota = lax.broadcasted_iota(jnp.int32, (seq, LANES), 0)
    lane = lax.broadcasted_iota(jnp.int32, (seq, LANES), 1)
    pair_low = lane % (dh // 2) < dh // 4
    by_pos = lane % dh < dh // 2
    n_tiles = seq // QUERY_TILE
    last_lane = lax.broadcasted_iota(jnp.int32, (1, toks), 1) == toks - 1

    def attend_row(b):
        ctx_b = ctx[b]
        m_b = jnp.sum(jnp.where(last_lane, m_v[pl.ds(b, 1), :].astype(jnp.float32), 0.0), axis=-1, keepdims=True)
        in_ctx = row_iota < ctx_b
        angle_m = m_b * freq[...]
        sin_m = jnp.sin(angle_m)
        sin_m = jnp.where(pair_low[0:1], -sin_m, sin_m)
        cos, sin = [jnp.where(by_pos, jnp.where(in_ctx, table[i, seq:2 * seq, :], trig_m), table[i, pl.ds(seq + 1 - ctx_b, seq), :])
                    for i, trig_m in enumerate([jnp.cos(angle_m), sin_m])]

        def rotate(x):
            swapped = jnp.where(pair_low, pltpu.roll(x, LANES - dh // 4, 1), pltpu.roll(x, dh // 4, 1))
            return x * cos + swapped * sin

        q = rotate(qkv[b, :, 0:LANES].astype(jnp.float32)) * (1.0 / math.sqrt(dh))
        k = rotate(qkv[b, :, LANES:2 * LANES].astype(jnp.float32))
        v_raw = qkv[b, :, 2 * LANES:3 * LANES]
        v = v_raw.astype(jnp.float32)
        k_v[b] = k.astype(jnp.bfloat16).T
        v_v[b] = v_raw.T

        heads = []
        for h in range(hl):
            mine = lane // dh == h
            heads.append([jnp.where(mine, x, 0.0).astype(jnp.bfloat16) for x in (q, k, v)])
        for qt in range(n_tiles):
            start = qt * QUERY_TILE
            rows_here = slice(start, start + QUERY_TILE)
            keys_here = max(CTX_MAX, start + QUERY_TILE)
            bound = jnp.maximum(ctx_b, row_iota[rows_here] + 1)
            total = None
            for q_h, k_h, v_h in heads:
                s = lax.dot_general(q_h[rows_here], k_h[:keys_here], NT, preferred_element_type=jnp.float32)
                tiles = []
                for kt in range(keys_here // LANES):
                    tile = s[:, kt * LANES:(kt + 1) * LANES]
                    last_key = (kt + 1) * LANES - 1
                    if last_key >= CTX_MIN and last_key > start:
                        tile = jnp.where(lane[rows_here] + kt * LANES < bound, tile, -jnp.inf)
                    tiles.append(tile)
                top = functools.reduce(jnp.maximum, tiles)
                top = jnp.max(top, axis=-1, keepdims=True)
                tiles = [jnp.exp(tile - top) for tile in tiles]
                norm = jnp.sum(functools.reduce(jnp.add, tiles), axis=-1, keepdims=True)
                inv = 1.0 / norm
                probs = jnp.concatenate([(tile * inv).astype(jnp.bfloat16) for tile in tiles], axis=1)
                o = jnp.dot(probs, v_h[:keys_here], preferred_element_type=jnp.float32)
                total = o if total is None else total + o
            owners = QUERY_TILE // toks
            cs[pl.ds(qt * owners, owners), b] = total.astype(jnp.bfloat16).reshape(owners, toks, LANES)

    def attend_chunk(kk, carry):
        some = qkv.at[pl.ds(kk * part, part), pl.ds(0, PLACES * toks)]
        pltpu.make_async_copy(some, some, q_recv.at[kk]).wait()

        def one_row(r, c):
            attend_row(kk * part + r)
            return c

        lax.fori_loop(0, part, one_row, 0)
        rows_k = pl.ds(kk * part, part)
        cols_me = pl.ds(pl.multiple_of(me * LANES, LANES), LANES)
        for step in far_first(n):
            dest = (me + step) % n
            pltpu.make_async_remote_copy(src_ref=cs.at[dest, rows_k], dst_ref=cr.at[rows_k, :, cols_me], send_sem=c_send,
                                         recv_sem=c_recv.at[kk], device_id={'sp': dest}, device_id_type=MESH).start()
        cr[rows_k, :, cols_me] = cs[me, rows_k]
        return carry

    attend_chunk(0, 0)
    lax.fori_loop(2, CHUNKS, far_chunk, 0)
    lax.fori_loop(1, CHUNKS, attend_chunk, 0)
    wd_copy.wait()

    def context_wait(kk):
        some = cr.at[pl.ds(kk * part, part), :, pl.ds(0, (n - 1) * LANES)]
        pltpu.make_async_copy(some, some, c_recv.at[kk]).wait()

    def dense_chunk(kk, carry):
        context_wait(kk)

        def columns(j, c):
            at = pl.ds(pl.multiple_of(j * DENSE_COLS, DENSE_COLS), DENSE_COLS)
            here = pl.ds(pl.multiple_of(kk * chunk, chunk), chunk)
            x = cr[pl.ds(kk * part, part)].reshape(chunk, width)
            dense = jnp.dot(x, wd_v[:, at], preferred_element_type=jnp.float32) + vecs[2:3, at]
            out_v[here, at] = (a_v[0, here, at].astype(jnp.float32) * ALPHA + dense).astype(jnp.bfloat16)
            return c

        lax.fori_loop(0, width // DENSE_COLS, columns, 0)
        return carry

    lax.fori_loop(0, CHUNKS - 1, dense_chunk, 0)
    rest_v[...] = a_v[0, pl.ds((CHUNKS - 1) * chunk, chunk), :].astype(jnp.float32) * ALPHA + vecs[2:3, :]
    for side in range(2):
        whole = a_v.at[0]
        pltpu.make_async_copy(whole, whole, a_send.at[side]).wait()
    pltpu.make_async_copy(fwd, fwd, f_send).wait()
    pltpu.make_async_copy(a_v.at[3], a_v.at[3], r_send).wait()

    @pl.when(me == n - 1)
    def _():
        for step in range(1, n):
            pltpu.make_async_copy(pos_v, m_v, m_send.at[step]).wait()

    sent = cs.at[pl.ds(0, n - 1)]
    pltpu.make_async_copy(sent, sent, c_send).wait()
    context_wait(CHUNKS - 1)
    last_v[...] = cr[pl.ds((CHUNKS - 1) * part, part)].reshape(chunk, width)


def finish_kernel(out_v, k_v, v_v, wd_v, last_v, rest_v, out, k_out, v_out, tail_v, sem, tail_sem):
    done = out_v.shape[0]
    chunk, width = last_v.shape
    copies = [pltpu.make_async_copy(k_v, k_out, sem.at[0]), pltpu.make_async_copy(v_v, v_out, sem.at[1]),
              pltpu.make_async_copy(out_v, out.at[pl.ds(0, done)], sem.at[2])]
    for copy in copies:
        copy.start()
    for j in range(width // DENSE_COLS):
        at = pl.ds(j * DENSE_COLS, DENSE_COLS)
        dense = jnp.dot(last_v[...], wd_v[:, at], preferred_element_type=jnp.float32)
        tail_v[:, at] = (rest_v[:, at] + dense).astype(jnp.bfloat16)
        copy = pltpu.make_async_copy(tail_v.at[:, at], out.at[pl.ds(done, chunk), at], tail_sem.at[j])
        copy.start()
        copies.append(copy)
    for copy in copies:
        copy.wait()


def solution(mesh):
    n = mesh.shape['sp']
    seq_spec = P('dp', 'sp', None)
    row_spec = P('dp', 'sp')
    head_spec = P('dp', None, 'sp', None)
    replicated = P()

    def local_block(hidden, pos_ids, block_ids, ctx_len, ln_gamma, ln_beta, w_qkv, b_qkv, w_dense, b_dense):
        rows, toks, width = hidden.shape
        heads, _, dh = b_qkv.shape
        hl = heads // n
        seq = n * toks
        tokens = rows * toks
        part = rows // CHUNKS
        chunk = part * toks
        cols = 3 * hl * dh
        bf16, f32 = jnp.bfloat16, jnp.float32
        w_t = jnp.transpose(w_qkv, (1, 2, 3, 0)).reshape(n, hl, 3, dh, width)
        half = dh // 2
        inv_freq = ROPE_BASE ** (-np.arange(0, half, 2).astype(np.float32) / half)
        freq = np.tile(inv_freq.astype(np.float32), LANES // inv_freq.shape[0])[None, :]
        vmem = pl.BlockSpec(memory_space=pltpu.VMEM)
        anywhere = pl.BlockSpec(memory_space=pl.ANY)
        kv_shape = (rows, hl * dh, seq)
        staged = pl.pallas_call(
            functools.partial(block_kernel, n, rows, toks, dh),
            out_shape=[pltpu.VMEM((tokens - chunk, width), bf16), pltpu.VMEM(kv_shape, bf16), pltpu.VMEM(kv_shape, bf16),
                       pltpu.VMEM((width, width), bf16), pltpu.VMEM((chunk, width), bf16), pltpu.VMEM((chunk, width), f32)],
            in_specs=[anywhere] * 10,
            out_specs=[vmem] * 6,
            scratch_shapes=[
                pltpu.VMEM((10, 3, hl, dh, width), bf16),
                pltpu.VMEM((4, tokens, width), bf16),
                pltpu.VMEM((PLACES, CHUNKS, part, toks, cols), bf16),
                pltpu.VMEM((rows, seq, cols), bf16),
                pltpu.VMEM((n, rows, toks, LANES), bf16),
                pltpu.VMEM((rows, toks, width), bf16),
                pltpu.VMEM((3, heads, dh), bf16),
                pltpu.VMEM((n, 1, cols), f32),
                pltpu.VMEM((width,), bf16),
                pltpu.VMEM((width,), bf16),
                pltpu.VMEM((width,), bf16),
                pltpu.VMEM((8, width), f32),
                pltpu.SMEM((rows,), jnp.int32),
                pltpu.VMEM((rows, toks), jnp.int32),
                pltpu.VMEM((rows, toks), jnp.int32),
                pltpu.VMEM((1, LANES), f32),
                pltpu.VMEM((2, 2 * seq + LANES, LANES), f32),
                pltpu.SemaphoreType.DMA((rows,)),
                pltpu.SemaphoreType.DMA((10,)),
                pltpu.SemaphoreType.DMA,
                pltpu.SemaphoreType.DMA((7,)),
                pltpu.SemaphoreType.DMA((2,)),
                pltpu.SemaphoreType.DMA((2, CHUNKS)),
                pltpu.SemaphoreType.DMA,
                pltpu.SemaphoreType.DMA((CHUNKS,)),
                pltpu.SemaphoreType.DMA,
                pltpu.SemaphoreType.DMA((CHUNKS,)),
                pltpu.SemaphoreType.DMA,
                pltpu.SemaphoreType.DMA((CHUNKS,)),
                pltpu.SemaphoreType.DMA((n,)),
                pltpu.SemaphoreType.DMA,
            ],
            compiler_params=pltpu.CompilerParams(collective_id=0, has_side_effects=True, vmem_limit_bytes=46 * 2**20),
            name='attention_block',
        )(hidden.reshape(tokens, width), w_t, jnp.transpose(b_qkv, (1, 0, 2)), w_dense, ln_gamma, ln_beta, b_dense, ctx_len, pos_ids, freq)
        out, k_out, v_out = pl.pallas_call(
            finish_kernel,
            out_shape=[jax.ShapeDtypeStruct((tokens, width), bf16)] + [jax.ShapeDtypeStruct(kv_shape, bf16)] * 2,
            in_specs=[vmem] * 6,
            out_specs=[anywhere] * 3,
            scratch_shapes=[pltpu.VMEM((chunk, width), bf16), pltpu.SemaphoreType.DMA((3,)), pltpu.SemaphoreType.DMA((width // DENSE_COLS,))],
            compiler_params=pltpu.CompilerParams(vmem_limit_bytes=4 * 2**20),
            name='finish_block',
        )(*staged)

        def to_heads(x):
            return jnp.transpose(x.reshape(rows, hl, dh, seq), (0, 3, 1, 2))

        return out.reshape(rows, toks, width), to_heads(k_out), to_heads(v_out)

    return jax.shard_map(local_block, mesh=mesh, in_specs=(seq_spec, row_spec, row_spec, P('dp'), replicated, replicated, replicated, replicated, replicated, replicated), out_specs=(seq_spec, head_spec, head_spec), check_vma=False)
```

```python
import functools
import math

import jax
import jax.numpy as jnp
import numpy as np
from jax import lax
from jax.experimental import pallas as pl
from jax.experimental.pallas import tpu as pltpu
from jax.sharding import PartitionSpec as P

ALPHA = math.sqrt(56.0)
ROPE_BASE = 10000.0
LN_EPS = 1e-5
CORES = 2
CHUNKS = 4
LANES = 128
QUERY_TILE = 128
CTX_MIN = 128
CTX_MAX = 384
FIRST_ROWS = 4
PLACES = 12
DENSE_COLS = 512
MESH = pl.DeviceIdType.MESH
NT = (((1,), (1,)), ((), ()))


def far_first(n):
    half = n // 2
    order = [half]
    for step in range(1, half):
        order += [half - step, half + step]
    return order


def block_kernel(n, rows, toks, dh, hidden, w_hbm, bq_hbm, wd_hbm, gamma_hbm, beta_hbm, bd_hbm, ctx_hbm, pos_hbm, freq_hbm,
                 out_v, k_v, v_v, wd_v, last_v, rest_v,
                 w_v, a_v, fwd, qkv, cs, cr, bq_v, bias, g_v, be_v, bd_v, vecs, ctx, pos_v, m_v, freq, table,
                 h_sem, w_sem, wd_sem, small_sem, a_send, a_recv, r_send, r_recv, f_send, q_recv, c_send, c_recv, m_send, m_recv):
    me = lax.axis_index('sp')
    chips = n // CORES
    chip, core = me // CORES, me % CORES
    part = rows // CHUNKS
    chunk = part * toks
    width = a_v.shape[2]
    seq = n * toks
    hl = w_hbm.shape[1]

    def device(chip_index, core_index):
        return {'sp': (chip_index % chips) * CORES + core_index}

    barrier = pltpu.get_barrier_semaphore()
    for step in range(1, n):
        pl.semaphore_signal(barrier, inc=1, device_id={'sp': (me + step) % n}, device_id_type=MESH)

    def row_at(r):
        return pl.ds(pl.multiple_of(r * toks, toks), toks)

    def hidden_copy(r):
        return pltpu.make_async_copy(hidden.at[row_at(r)], a_v.at[0, row_at(r)], h_sem.at[r])

    small = [(gamma_hbm, g_v), (beta_hbm, be_v), (bd_hbm, bd_v), (bq_hbm, bq_v), (ctx_hbm, ctx), (pos_hbm, pos_v), (freq_hbm, freq)]
    small_copies = [pltpu.make_async_copy(src, dst, small_sem.at[i]) for i, (src, dst) in enumerate(small)]
    hidden_copy(0).start()
    for copy in small_copies[:2]:
        copy.start()
    for r in range(1, rows):
        hidden_copy(r).start()
    for copy in small_copies[2:]:
        copy.start()
    for i in range(2):
        small_copies[i].wait()
        vecs[i:i + 1, :] = small[i][1][...].astype(jnp.float32)[None, :]

    def a_copy(start, size, k, side):
        peer = device(chip + 1 - 2 * side + chips, core)
        at = pl.ds(start, size)
        return pltpu.make_async_remote_copy(src_ref=a_v.at[0, at], dst_ref=a_v.at[1 + side, at],
                                            send_sem=a_send.at[side], recv_sem=a_recv.at[side, k],
                                            device_id=peer, device_id_type=MESH)

    def norm_row(r, carry):
        hidden_copy(r).wait()
        x = a_v[0, row_at(r), :].astype(jnp.float32)
        mean = jnp.mean(x, axis=-1, keepdims=True)
        centered = x - mean
        var = jnp.mean(jnp.square(centered), axis=-1, keepdims=True)
        a_v[0, row_at(r), :] = (centered * lax.rsqrt(var + LN_EPS) * vecs[0:1, :] + vecs[1:2, :]).astype(jnp.bfloat16)
        return carry

    def send_row(r):
        for side in range(2):
            a_copy(pl.multiple_of(r * toks, toks), toks, r // part, side).start()

    def norm_send_row(r, carry):
        norm_row(r, carry)
        send_row(r)
        return carry

    norm_row(0, 0)
    pl.semaphore_wait(barrier, n - 1)
    send_row(0)
    lax.fori_loop(1, FIRST_ROWS, norm_send_row, 0)

    def weight_copy(slot, block):
        for h in range(hl):
            for t in range(3):
                pltpu.make_async_copy(w_hbm.at[block, h, t], w_v.at[slot, t, h], w_sem.at[slot]).start()

    weight_blocks = [(step, kore) for step in (0, 1, 2, -1, -2) for kore in range(CORES)]
    for slot, (step, kore) in enumerate(weight_blocks):
        weight_copy(slot, ((chip + step + chips) % chips) * CORES + kore)
    wd_copy = pltpu.make_async_copy(wd_hbm, wd_v, wd_sem)
    wd_copy.start()
    lax.fori_loop(FIRST_ROWS, 2 * part, norm_send_row, 0)
    lax.fori_loop(2 * part, rows, norm_row, 0)

    for copy in small_copies[2:]:
        copy.wait()
    vecs[2:3, :] = bd_v[...].astype(jnp.float32)[None, :]
    raw = bq_v[...].astype(jnp.float32)
    for d in range(n):
        for t in range(3):
            bias[d, :, t * hl * dh:(t + 1) * hl * dh] = jnp.concatenate([raw[t, hl * d + h:hl * d + h + 1] for h in range(hl)], axis=1)

    @pl.when(me == n - 1)
    def _():
        for step in range(1, n):
            pltpu.make_async_remote_copy(src_ref=pos_v, dst_ref=m_v, send_sem=m_send.at[step], recv_sem=m_recv,
                                         device_id={'sp': (me + step) % n}, device_id_type=MESH).start()
        m_v[...] = pos_v[...]

    def project(source, k, slot, count, block):
        a = a_v[source, pl.ds(pl.multiple_of(k * chunk, chunk), chunk), :]
        w = w_v[pl.ds(slot, count)].reshape(count * 3 * hl * dh, width)
        acc = lax.dot_general(a, w, NT, preferred_element_type=jnp.float32)
        cols = 3 * hl * dh
        return [(acc[:, i * cols:(i + 1) * cols] + bias[block + i]).astype(jnp.bfloat16).reshape(part, toks, cols) for i in range(count)]

    def owner_at(k, owner):
        return pl.ds(k * part, part), pl.ds(pl.multiple_of(owner * toks, toks), toks)

    def send(value, k, slot, owner, dest):
        fwd[slot, k] = value
        at = owner_at(k, owner)
        pltpu.make_async_remote_copy(src_ref=fwd.at[slot, k], dst_ref=qkv.at[at[0], at[1]], send_sem=f_send, recv_sem=q_recv.at[k],
                                     device_id=dest, device_id_type=MESH).start()

    def job(source, k, slot, target, owner, place, apart, own):
        values = project(source, k, slot, CORES, target * CORES)
        for h in range(CORES):
            keep = jnp.logical_and(own == 1, core == h)

            @pl.when(keep)
            def _():
                at = owner_at(k, owner)
                qkv[at[0], at[1], :] = values[h]

            @pl.when(jnp.logical_not(keep))
            def _():
                send(values[h], k, place + h * apart, owner, device(target, h))

    def wait_weights(slot):
        pltpu.make_async_copy(w_v.at[slot], w_v.at[slot], w_sem.at[slot]).wait()

    table_rows = table.shape[1]

    def table_block(i, carry):
        at = pl.ds(pl.multiple_of(i * LANES, LANES), LANES)
        index = lax.broadcasted_iota(jnp.int32, (LANES, LANES), 0) + (i * LANES - seq)
        angle = jnp.maximum(index, 0).astype(jnp.float32) * freq[...]
        quarter = lax.broadcasted_iota(jnp.int32, (LANES, LANES), 1) % (dh // 2) < dh // 4
        sin = jnp.sin(angle)
        table[0, at, :] = jnp.cos(angle)
        table[1, at, :] = jnp.where(quarter, -sin, sin)
        return carry

    lax.fori_loop(0, table_rows // LANES, table_block, 0)
    for slot in range(CORES):
        wait_weights(slot)

    def chip_at(offset):
        return (chip + offset + chips) % chips

    def chunk_at(k):
        return pl.ds(pl.multiple_of(k * chunk, chunk), chunk)

    def own_chunk(k, carry):
        job(0, k, 0, chip, me, 0, 0, 1)
        return carry

    def relay(k):
        odd = k % 2
        return pltpu.make_async_remote_copy(src_ref=a_v.at[1 + odd, chunk_at(k)], dst_ref=a_v.at[3, chunk_at(k)],
                                            send_sem=r_send, recv_sem=r_recv.at[k],
                                            device_id=device(chip_at(1 - 2 * odd), core), device_id_type=MESH)

    def near_chunk(k, carry):
        odd = k % 2
        for side in range(2):
            a_copy(pl.multiple_of(k * chunk, chunk), chunk, k, side).wait_recv()
        relay(k).start()

        def one(i, c):
            own = i // 2
            step = (2 - i) * (1 - own)
            source = (1 - own) * (2 - odd) + own * ((3 - i) * (1 + odd) + (i - 2) * (2 - odd))
            slot = (1 - own) * (CORES + CORES * (2 * (1 - odd) + step - 1))
            place = (1 - own) * (4 + CORES * (step - 1)) + own * source
            owner = chip_at(2 * source - 3) * CORES + core
            job(source, k, slot, chip_at((2 * odd - 1) * step), owner, place, 1 - own, own)
            return c

        lax.fori_loop(0, 4, one, 0)
        return carry

    def far_chunk(k, carry):
        odd = k % 2
        there = a_v.at[3, chunk_at(k)]
        pltpu.make_async_copy(there, there, r_recv.at[k]).wait()
        owner = chip_at(4 * odd - 2) * CORES + core

        def one(i, c):
            own = i // 2
            step = 2 - i
            slot = (1 - own) * (CORES + CORES * (2 * odd + step - 1))
            place = (1 - own) * (8 + CORES * (step - 1)) + own * 3
            job(3, k, slot, chip_at((1 - 2 * odd) * step), owner, place, 1 - own, own)
            return c

        lax.fori_loop(0, 3, one, 0)
        return carry

    lax.fori_loop(0, CHUNKS, own_chunk, 0)
    for slot in range(CORES, len(weight_blocks)):
        wait_weights(slot)
    near_chunk(0, 0)
    for k in range(2, CHUNKS):
        for side in range(2):
            a_copy(k * chunk, chunk, k, side).start()
    near_chunk(1, 0)
    far_chunk(0, 0)
    lax.fori_loop(2, CHUNKS, near_chunk, 0)
    far_chunk(1, 0)

    @pl.when(me != n - 1)
    def _():
        pltpu.make_async_copy(pos_v, m_v, m_recv).wait()

    row_iota = lax.broadcasted_iota(jnp.int32, (seq, LANES), 0)
    lane = lax.broadcasted_iota(jnp.int32, (seq, LANES), 1)
    pair_low = lane % (dh // 2) < dh // 4
    by_pos = lane % dh < dh // 2
    n_tiles = seq // QUERY_TILE
    last_lane = lax.broadcasted_iota(jnp.int32, (1, toks), 1) == toks - 1

    def attend_row(b):
        ctx_b = ctx[b]
        m_b = jnp.sum(jnp.where(last_lane, m_v[pl.ds(b, 1), :].astype(jnp.float32), 0.0), axis=-1, keepdims=True)
        in_ctx = row_iota < ctx_b
        angle_m = m_b * freq[...]
        sin_m = jnp.sin(angle_m)
        sin_m = jnp.where(pair_low[0:1], -sin_m, sin_m)
        cos, sin = [jnp.where(by_pos, jnp.where(in_ctx, table[i, seq:2 * seq, :], trig_m), table[i, pl.ds(seq + 1 - ctx_b, seq), :])
                    for i, trig_m in enumerate([jnp.cos(angle_m), sin_m])]

        def rotate(x):
            swapped = jnp.where(pair_low, pltpu.roll(x, LANES - dh // 4, 1), pltpu.roll(x, dh // 4, 1))
            return x * cos + swapped * sin

        q = rotate(qkv[b, :, 0:LANES].astype(jnp.float32)) * (1.0 / math.sqrt(dh))
        k = rotate(qkv[b, :, LANES:2 * LANES].astype(jnp.float32))
        v_raw = qkv[b, :, 2 * LANES:3 * LANES]
        v = v_raw.astype(jnp.float32)
        k_v[b] = k.astype(jnp.bfloat16).T
        v_v[b] = v_raw.T

        heads = []
        for h in range(hl):
            mine = lane // dh == h
            heads.append([jnp.where(mine, x, 0.0).astype(jnp.bfloat16) for x in (q, k, v)])
        for qt in range(n_tiles):
            start = qt * QUERY_TILE
            rows_here = slice(start, start + QUERY_TILE)
            keys_here = max(CTX_MAX, start + QUERY_TILE)
            bound = jnp.maximum(ctx_b, row_iota[rows_here] + 1)
            total = None
            for q_h, k_h, v_h in heads:
                s = lax.dot_general(q_h[rows_here], k_h[:keys_here], NT, preferred_element_type=jnp.float32)
                tiles = []
                for kt in range(keys_here // LANES):
                    tile = s[:, kt * LANES:(kt + 1) * LANES]
                    last_key = (kt + 1) * LANES - 1
                    if last_key >= CTX_MIN and last_key > start:
                        tile = jnp.where(lane[rows_here] + kt * LANES < bound, tile, -jnp.inf)
                    tiles.append(tile)
                top = functools.reduce(jnp.maximum, tiles)
                top = jnp.max(top, axis=-1, keepdims=True)
                tiles = [jnp.exp(tile - top) for tile in tiles]
                norm = jnp.sum(functools.reduce(jnp.add, tiles), axis=-1, keepdims=True)
                inv = 1.0 / norm
                probs = jnp.concatenate([(tile * inv).astype(jnp.bfloat16) for tile in tiles], axis=1)
                o = jnp.dot(probs, v_h[:keys_here], preferred_element_type=jnp.float32)
                total = o if total is None else total + o
            owners = QUERY_TILE // toks
            cs[pl.ds(qt * owners, owners), b] = total.astype(jnp.bfloat16).reshape(owners, toks, LANES)

    def attend_chunk(kk, carry):
        some = qkv.at[pl.ds(kk * part, part), pl.ds(0, PLACES * toks)]
        pltpu.make_async_copy(some, some, q_recv.at[kk]).wait()

        def one_row(r, c):
            attend_row(kk * part + r)
            return c

        lax.fori_loop(0, part, one_row, 0)
        rows_k = pl.ds(kk * part, part)
        cols_me = pl.ds(pl.multiple_of(me * LANES, LANES), LANES)
        for step in far_first(n):
            dest = (me + step) % n
            pltpu.make_async_remote_copy(src_ref=cs.at[dest, rows_k], dst_ref=cr.at[rows_k, :, cols_me], send_sem=c_send,
                                         recv_sem=c_recv.at[kk], device_id={'sp': dest}, device_id_type=MESH).start()
        cr[rows_k, :, cols_me] = cs[me, rows_k]
        return carry

    attend_chunk(0, 0)
    lax.fori_loop(2, CHUNKS, far_chunk, 0)
    lax.fori_loop(1, CHUNKS, attend_chunk, 0)
    wd_copy.wait()

    def context_wait(kk):
        some = cr.at[pl.ds(kk * part, part), :, pl.ds(0, (n - 1) * LANES)]
        pltpu.make_async_copy(some, some, c_recv.at[kk]).wait()

    def dense_chunk(kk, carry):
        context_wait(kk)

        def columns(j, c):
            at = pl.ds(pl.multiple_of(j * DENSE_COLS, DENSE_COLS), DENSE_COLS)
            here = pl.ds(pl.multiple_of(kk * chunk, chunk), chunk)
            x = cr[pl.ds(kk * part, part)].reshape(chunk, width)
            dense = jnp.dot(x, wd_v[:, at], preferred_element_type=jnp.float32) + vecs[2:3, at]
            out_v[here, at] = (a_v[0, here, at].astype(jnp.float32) * ALPHA + dense).astype(jnp.bfloat16)
            return c

        lax.fori_loop(0, width // DENSE_COLS, columns, 0)
        return carry

    lax.fori_loop(0, CHUNKS - 1, dense_chunk, 0)
    rest_v[...] = a_v[0, pl.ds((CHUNKS - 1) * chunk, chunk), :].astype(jnp.float32) * ALPHA + vecs[2:3, :]
    for side in range(2):
        whole = a_v.at[0]
        pltpu.make_async_copy(whole, whole, a_send.at[side]).wait()
    pltpu.make_async_copy(fwd, fwd, f_send).wait()
    pltpu.make_async_copy(a_v.at[3], a_v.at[3], r_send).wait()

    @pl.when(me == n - 1)
    def _():
        for step in range(1, n):
            pltpu.make_async_copy(pos_v, m_v, m_send.at[step]).wait()

    sent = cs.at[pl.ds(0, n - 1)]
    pltpu.make_async_copy(sent, sent, c_send).wait()
    context_wait(CHUNKS - 1)
    last_v[...] = cr[pl.ds((CHUNKS - 1) * part, part)].reshape(chunk, width)


def finish_kernel(out_v, k_v, v_v, wd_v, last_v, rest_v, out, k_out, v_out, tail_v, sem, tail_sem):
    done = out_v.shape[0]
    chunk, width = last_v.shape
    copies = [pltpu.make_async_copy(k_v, k_out, sem.at[0]), pltpu.make_async_copy(v_v, v_out, sem.at[1]),
              pltpu.make_async_copy(out_v, out.at[pl.ds(0, done)], sem.at[2])]
    for copy in copies:
        copy.start()
    for j in range(width // DENSE_COLS):
        at = pl.ds(j * DENSE_COLS, DENSE_COLS)
        dense = jnp.dot(last_v[...], wd_v[:, at], preferred_element_type=jnp.float32)
        tail_v[:, at] = (rest_v[:, at] + dense).astype(jnp.bfloat16)
        copy = pltpu.make_async_copy(tail_v.at[:, at], out.at[pl.ds(done, chunk), at], tail_sem.at[j])
        copy.start()
        copies.append(copy)
    for copy in copies:
        copy.wait()


def solution(mesh):
    n = mesh.shape['sp']
    seq_spec = P('dp', 'sp', None)
    row_spec = P('dp', 'sp')
    head_spec = P('dp', None, 'sp', None)
    replicated = P()

    def local_block(hidden, pos_ids, block_ids, ctx_len, ln_gamma, ln_beta, w_qkv, b_qkv, w_dense, b_dense):
        rows, toks, width = hidden.shape
        heads, _, dh = b_qkv.shape
        hl = heads // n
        seq = n * toks
        tokens = rows * toks
        part = rows // CHUNKS
        chunk = part * toks
        cols = 3 * hl * dh
        bf16, f32 = jnp.bfloat16, jnp.float32
        w_t = jnp.transpose(w_qkv, (1, 2, 3, 0)).reshape(n, hl, 3, dh, width)
        half = dh // 2
        inv_freq = ROPE_BASE ** (-np.arange(0, half, 2).astype(np.float32) / half)
        freq = np.tile(inv_freq.astype(np.float32), LANES // inv_freq.shape[0])[None, :]
        vmem = pl.BlockSpec(memory_space=pltpu.VMEM)
        anywhere = pl.BlockSpec(memory_space=pl.ANY)
        kv_shape = (rows, hl * dh, seq)
        staged = pl.pallas_call(
            functools.partial(block_kernel, n, rows, toks, dh),
            out_shape=[pltpu.VMEM((tokens - chunk, width), bf16), pltpu.VMEM(kv_shape, bf16), pltpu.VMEM(kv_shape, bf16),
                       pltpu.VMEM((width, width), bf16), pltpu.VMEM((chunk, width), bf16), pltpu.VMEM((chunk, width), f32)],
            in_specs=[anywhere] * 10,
            out_specs=[vmem] * 6,
            scratch_shapes=[
                pltpu.VMEM((10, 3, hl, dh, width), bf16),
                pltpu.VMEM((4, tokens, width), bf16),
                pltpu.VMEM((PLACES, CHUNKS, part, toks, cols), bf16),
                pltpu.VMEM((rows, seq, cols), bf16),
                pltpu.VMEM((n, rows, toks, LANES), bf16),
                pltpu.VMEM((rows, toks, width), bf16),
                pltpu.VMEM((3, heads, dh), bf16),
                pltpu.VMEM((n, 1, cols), f32),
                pltpu.VMEM((width,), bf16),
                pltpu.VMEM((width,), bf16),
                pltpu.VMEM((width,), bf16),
                pltpu.VMEM((8, width), f32),
                pltpu.SMEM((rows,), jnp.int32),
                pltpu.VMEM((rows, toks), jnp.int32),
                pltpu.VMEM((rows, toks), jnp.int32),
                pltpu.VMEM((1, LANES), f32),
                pltpu.VMEM((2, 2 * seq + LANES, LANES), f32),
                pltpu.SemaphoreType.DMA((rows,)),
                pltpu.SemaphoreType.DMA((10,)),
                pltpu.SemaphoreType.DMA,
                pltpu.SemaphoreType.DMA((7,)),
                pltpu.SemaphoreType.DMA((2,)),
                pltpu.SemaphoreType.DMA((2, CHUNKS)),
                pltpu.SemaphoreType.DMA,
                pltpu.SemaphoreType.DMA((CHUNKS,)),
                pltpu.SemaphoreType.DMA,
                pltpu.SemaphoreType.DMA((CHUNKS,)),
                pltpu.SemaphoreType.DMA,
                pltpu.SemaphoreType.DMA((CHUNKS,)),
                pltpu.SemaphoreType.DMA((n,)),
                pltpu.SemaphoreType.DMA,
            ],
            compiler_params=pltpu.CompilerParams(collective_id=0, has_side_effects=True, vmem_limit_bytes=46 * 2**20),
            name='attention_block',
        )(hidden.reshape(tokens, width), w_t, jnp.transpose(b_qkv, (1, 0, 2)), w_dense, ln_gamma, ln_beta, b_dense, ctx_len, pos_ids, freq)
        out, k_out, v_out = pl.pallas_call(
            finish_kernel,
            out_shape=[jax.ShapeDtypeStruct((tokens, width), bf16)] + [jax.ShapeDtypeStruct(kv_shape, bf16)] * 2,
            in_specs=[vmem] * 6,
            out_specs=[anywhere] * 3,
            scratch_shapes=[pltpu.VMEM((chunk, width), bf16), pltpu.SemaphoreType.DMA((3,)), pltpu.SemaphoreType.DMA((width // DENSE_COLS,))],
            compiler_params=pltpu.CompilerParams(vmem_limit_bytes=4 * 2**20),
            name='finish_block',
        )(*staged)

        def to_heads(x):
            return jnp.transpose(x.reshape(rows, hl, dh, seq), (0, 3, 1, 2))

        return out.reshape(rows, toks, width), to_heads(k_out), to_heads(v_out)

    return jax.shard_map(local_block, mesh=mesh, in_specs=(seq_spec, row_spec, row_spec, P('dp'), replicated, replicated, replicated, replicated, replicated, replicated), out_specs=(seq_spec, head_spec, head_spec), check_vma=False)
```
